32 devices in a mesh: group: 2 (over x), seq: 8 (over z, y), tensor: 2 (over core).
Axes of the slice: x: 2, y: 2, z: 4, core: 2. Of those that a mesh axis runs over, the one named last changes fastest.
Arguments:
- hidden: bfloat16 [6, 1024, 8192], P('group', 'seq', 'tensor'), parts along dimension 0, may hold values from -64 to 64
- norm_gain: bfloat16 [8192], replicated, may hold values from 0.099609375 to 1.8984375
- w_kv: bfloat16 [8192, 1024], P(None, 'tensor'), may hold values from -0.0625 to 0.0625
- lengths: int32 [6], P('group'), parts along dimension 0, may hold values from 512 to 1024
- page_table: int32 [6, 8], P('group', 'seq'), parts along dimension 0, may hold values from 0 to 63, as said below
Outputs:
- kv_cache: bfloat16 [128, 128, 1024], P(('group', 'seq'), None, 'tensor'), parts along dimension 0
The draws below stay inside these ranges and needn't reach their ends.
There are 2 independent parts, one for each index of `group`. The reference program is written for one: setup_inputs(seed, part) draws one part's arguments, and reference() takes and returns one part's arrays. A program takes and returns all parts, laid end to end along the dimension named above; an argument that names none is the same for every part. Nothing has to cross between parts.
Inputs may be any that keep to these rules, and one draw needn't show every extreme that they name: `page_table`: entries are distinct; page p is held by index p // 8 of seq in its slot p % 8. In every draw some index of seq holds 8 pages whose blocks all start below the window's length, and some index of seq sends all its 3 blocks to that one holder.
All inputs are finite; a program needn't handle non-finite values.
Results may differ from the reference program's by a relative error of at most 0.0049.
Values may be sent and summed in bfloat16 or wider, within the bound.
A program may use at most 128 MiB of HBM per device.

```python
import jax
import jax.numpy as jnp
from jax import lax

D = 8192
HD = 128
KVH = 4
BLOCK = 128
SEQS = 3
BPD = 1
SLOTS = 8
LENGTH = 1024
BLOCKS = 8
PAGES = 64
N_SEQ = 8


def draw_hidden(key, part):
    base = jax.random.fold_in(key, 11)
    key_base, key_rows, key_cols = jax.random.split(base, 3)
    shape = (SEQS, LENGTH, D)
    col_scale = jnp.exp(jax.random.uniform(key_cols, (1, 1, D), jnp.float32, -1.15, 1.15))
    row_scale = jnp.exp(jax.random.uniform(key_rows, (SEQS, LENGTH, 1), jnp.float32, -1.15, 1.15))
    values = jax.random.truncated_normal(key_base, -5.0, 5.0, shape, jnp.float32)
    return (values * row_scale * col_scale).astype(jnp.bfloat16)


def draw_page_table(key, part):
    base = jax.random.fold_in(key, 23)
    key_owner, key_sender, key_bias, key_spread, key_tail, key_order = jax.random.split(base, 6)
    total_blocks = SEQS * BLOCKS
    favoured = jax.random.randint(key_owner, (), 0, N_SEQ)
    sender = jax.random.randint(key_sender, (), 0, N_SEQ // 2)
    owner_bias = jax.random.randint(key_bias, (N_SEQ,), 0, 4)
    page_owner = jnp.arange(PAGES, dtype=jnp.int32) // SLOTS
    spread = jax.random.permutation(key_spread, PAGES).astype(jnp.int32)
    scores = jnp.where(page_owner == favoured, 8 * PAGES, 0) + owner_bias[page_owner] * PAGES + spread
    chosen = lax.top_k(scores, total_blocks)[1].astype(jnp.int32)
    head_pages = chosen[:SLOTS]
    tail_pages = jax.random.permutation(key_tail, chosen[SLOTS:])
    page_list = jnp.concatenate([head_pages, tail_pages]).astype(jnp.int32)
    block_device = jnp.arange(total_blocks, dtype=jnp.int32) % BLOCKS // BPD
    ranking = jnp.where(block_device == sender, 0, jnp.where(block_device < N_SEQ // 2, 1, 2))
    order_key = ranking * total_blocks + jax.random.permutation(key_order, total_blocks).astype(jnp.int32)
    ordering = jnp.argsort(order_key, stable=True)
    table = jnp.zeros((total_blocks,), jnp.int32).at[ordering].set(page_list)
    return table.reshape(SEQS, BLOCKS)


def steps_of(rng, extent, cuts, smallest, largest):
    def one(dim, blocks):
        steps = jax.random.uniform(jax.random.fold_in(jax.random.fold_in(rng, 6), dim), (blocks,), jnp.float32, smallest / len(cuts), largest / len(cuts))
        return jnp.repeat(jnp.exp(steps), extent[dim] // blocks).reshape((-1,) + (1,) * (len(extent) - dim - 1))

    loudness = one(*cuts[0])
    for cut in cuts[1:]:
        loudness = loudness * one(*cut)
    return loudness


def bell_draw(key, extent, width, bound, cuts=(), held_as=jnp.bfloat16):
    entries = jax.random.normal(key, extent, jnp.float32) * width
    if len(cuts) > 0:
        entries = steps_of(key, extent, cuts, -0.22, 0.18) * entries
    return jnp.clip(entries, min=-bound, max=bound).astype(held_as)


def setup_inputs(seed: int = 0, part: int = 0) -> dict:
    arg_keys = jax.random.split(jax.random.key(seed), 6)
    own_keys = jax.random.split(jax.random.fold_in(arg_keys[5], part), 6)
    hidden = draw_hidden(jax.random.fold_in(jax.random.fold_in(arg_keys[5], part), 71), part)
    norm_gain = jnp.clip(1.0 + 0.18 * jax.random.normal(arg_keys[1], (D,), jnp.float32), 0.099609375, 1.8984375).astype(jnp.bfloat16)
    w_kv = bell_draw(arg_keys[2], (D, KVH * 2 * HD), D ** -0.5, 0.0625, ((1, 2),))
    lengths = jax.random.randint(own_keys[3], (SEQS,), LENGTH // 2, LENGTH + 1).astype(jnp.int32)
    page_table = draw_page_table(jax.random.fold_in(jax.random.fold_in(arg_keys[5], part), 71), part)
    return {"hidden": hidden, "norm_gain": norm_gain, "w_kv": w_kv, "lengths": lengths, "page_table": page_table}


epsilon = 1e-05
rope_base = 500000.0

def rotate(key_heads, positions):
    half_dim = key_heads.shape[-1] // 2
    inv_freq = rope_base ** (-2.0 * jnp.arange(half_dim, dtype=jnp.float32) / key_heads.shape[-1])
    angles = positions.astype(jnp.float32)[:, None] * inv_freq[None, :]
    cosine = jnp.cos(angles)[:, None, :]
    sine = jnp.sin(angles)[:, None, :]
    first = key_heads[..., :half_dim]
    second = key_heads[..., half_dim:]
    return jnp.concatenate([first * cosine - second * sine, second * cosine + first * sine], axis=-1)

def reference(hidden, norm_gain, w_kv, lengths, page_table):
    wide_f32 = hidden.astype(jnp.float32)
    mean_sq = lax.optimization_barrier(jnp.sum(wide_f32 * wide_f32, axis=-1, keepdims=True)) / D
    normed = (wide_f32 * lax.rsqrt(mean_sq + epsilon) * norm_gain.astype(jnp.float32)).astype(jnp.bfloat16)
    projected = jnp.dot(normed.reshape(-1, D), w_kv, preferred_element_type=jnp.float32)
    projected = projected.reshape(SEQS, LENGTH, KVH, 2, HD)
    positions = jnp.arange(LENGTH, dtype=jnp.int32)
    rotated = rotate(projected[:, :, :, 0, :], positions)
    stacked = jnp.stack([rotated, projected[:, :, :, 1, :]], axis=3)
    living = (positions[None, :] < lengths[:, None])[:, :, None, None, None]
    restored = jnp.where(living, stacked, jnp.zeros((), jnp.float32)).astype(jnp.bfloat16)
    restored = restored.reshape(SEQS * BLOCKS, BLOCK, KVH * 2 * HD)
    kv_cache = jnp.zeros((PAGES, BLOCK, KVH * 2 * HD), jnp.bfloat16)
    return kv_cache.at[page_table.reshape(-1).astype(jnp.int32)].set(restored)
```

```python
import functools

import jax
import jax.numpy as jnp
import numpy as np
from jax import lax
from jax.experimental import pallas as pl
from jax.experimental.pallas import tpu as pltpu
from jax.sharding import PartitionSpec as P

HD = 128
BLOCK = 128
SLOTS = 8
PIECES = 8
PLANE = 4

epsilon = 1e-05
rope_base = 500000.0
MESH = pl.DeviceIdType.MESH


def kernel(
    depth, across, halves,
    hidden, gain, w_kv, lengths, table, freq,
    out,
    h_own, h_peer, w_buf, buf, id_row, table_all, table_s,
    h_sem, hs_sem, hr_sem, w_sem, ms_sem, mr_sem, t_sem,
    us_sem, ur_sem, ds_sem, dr_sem, ys_sem, yr_sem,
):
    n = depth * across
    seqs, rows, local = h_own.shape
    piece = w_buf.shape[1]
    per_half = PIECES // 2
    full = 2 * local
    me = lax.axis_index("seq")
    side = lax.axis_index("tensor")
    z = me // across
    y = me % across
    y_peer = z * across + (across - 1 - y)

    own_copies = [pltpu.make_async_copy(hidden.at[s], h_own.at[s], h_sem.at[s]) for s in range(seqs)]

    def w_copy(slot):
        half = side if slot < per_half else 1 - side
        index = half * per_half + slot % per_half
        return pltpu.make_async_copy(
            w_kv.at[pl.ds(index * piece, piece), :], w_buf.at[slot], w_sem.at[slot]
        )

    w_copies = [w_copy(i) for i in range(PIECES)]
    own_copies[0].start()
    for c in w_copies[:per_half]:
        c.start()

    id_lane = lax.broadcasted_iota(jnp.int32, (1, HD), 1)
    ids = jnp.full((1, HD), -1, jnp.int32)
    for s in range(seqs):
        ids = jnp.where(id_lane == s, table[s], ids)
    id_row[...] = ids

    barrier = pltpu.get_barrier_semaphore()
    pl.semaphore_signal(barrier, inc=1, device_id={"tensor": 1 - side}, device_id_type=MESH)
    for step in range(1, n):
        pl.semaphore_signal(
            barrier, inc=1, device_id={"seq": lax.rem(me + step, n)}, device_id_type=MESH
        )
    pl.semaphore_wait(barrier, n)

    def peer_copy(s, part):
        cut = pl.ds(part * piece, piece)
        i = s * per_half + part
        return pltpu.make_async_remote_copy(
            src_ref=hidden.at[s, :, cut], dst_ref=h_peer.at[s, :, cut],
            send_sem=hs_sem.at[i], recv_sem=hr_sem.at[i],
            device_id={"tensor": 1 - side}, device_id_type=MESH,
        )

    peer_copies = [[peer_copy(s, part) for part in range(per_half)] for s in range(seqs)]
    for c in peer_copies[0]:
        c.start()
    for c in w_copies[per_half:]:
        c.start()
    for s in range(1, seqs):
        own_copies[s].start()
        for c in peer_copies[s]:
            c.start()

    def id_copy(step):
        return pltpu.make_async_remote_copy(
            src_ref=id_row, dst_ref=table_all.at[me],
            send_sem=ms_sem.at[step - 1], recv_sem=mr_sem.at[step - 1],
            device_id={"seq": lax.rem(me + step, n)}, device_id_type=MESH,
        )

    def id_landed(step):
        return pltpu.make_async_remote_copy(
            src_ref=id_row, dst_ref=table_all.at[lax.rem(me + n - step, n)],
            send_sem=ms_sem.at[step - 1], recv_sem=mr_sem.at[step - 1],
            device_id={"seq": lax.rem(me + step, n)}, device_id_type=MESH,
        )

    for step in range(1, n):
        id_copy(step).start()
    table_all[me] = ids

    position = me * rows + lax.broadcasted_iota(jnp.int32, (rows, 1), 0)
    angle = position.astype(jnp.float32) * freq[...]
    cosine = jnp.cos(angle)
    lane = lax.broadcasted_iota(jnp.int32, (rows, HD), 1)
    sine = jnp.where(lane < HD // 2, -1.0, 1.0) * jnp.sin(angle)

    count = seqs * halves if halves else 1
    extra = 1 if across == 2 else 0
    stride = count + extra

    def unit(dev, u):
        if not halves:
            return buf.at[dev]
        part = rows // halves
        return buf.at[dev, u // halves, pl.ds((u % halves) * part, part), :]

    def send(ref, ssem, rsem, dev):
        return pltpu.make_async_remote_copy(
            src_ref=ref, dst_ref=ref, send_sem=ssem, recv_sem=rsem,
            device_id={"seq": dev}, device_id_type=MESH,
        )

    def up_send(k, u):
        ref = unit(me - k * across, u) if u < count else unit(y_peer - k * across, 0)
        i = k * stride + u
        return send(ref, us_sem.at[i], ur_sem.at[i], me + across)

    def down_send(k, u):
        ref = unit(me + k * across, u) if u < count else unit(y_peer + k * across, 0)
        i = k * stride + u
        return send(ref, ds_sem.at[i], dr_sem.at[i], me - across)

    def up_recv(k, u):
        far = (k + 1) * across
        ref = unit(me - far, u) if u < count else unit(y_peer - far, 0)
        i = k * stride + u
        return send(ref, us_sem.at[i], ur_sem.at[i], me - across)

    def down_recv(k, u):
        far = (k + 1) * across
        ref = unit(me + far, u) if u < count else unit(y_peer + far, 0)
        i = k * stride + u
        return send(ref, ds_sem.at[i], dr_sem.at[i], me + across)

    def side_copy(shift, u, base, mine):
        i = base + u
        ref = unit((me if mine else y_peer) + shift * across, u)
        return send(ref, ys_sem.at[i], yr_sem.at[i], y_peer)

    def up_base(k):
        return count * (1 + k)

    def down_base(k):
        return count * (depth + k)

    has_up = z + 1 < depth
    has_down = z >= 1

    def send_own(u):
        @pl.when(has_up)
        def _():
            up_send(0, u).start()

        @pl.when(has_down)
        def _():
            down_send(0, u).start()

        if across == 2:
            side_copy(0, u, 0, True).start()

    def project(first, many):
        size = many * rows
        acc = jnp.zeros((size, w_buf.shape[2]), jnp.float32)
        squares = jnp.zeros((size, HD), jnp.float32)
        for s in range(first, first + many):
            own_copies[s].wait()
        for slot in range(PIECES):
            if slot >= per_half:
                for s in range(first, first + many):
                    peer_copies[s][slot - per_half].wait_recv()
            if first == 0:
                w_copies[slot].wait()
            src = h_own if slot < per_half else h_peer
            half = side if slot < per_half else 1 - side
            at = (slot % per_half) * piece
            raw = src[pl.ds(first, many), :, pl.ds(at, piece)].reshape(size, piece)
            wide = raw.astype(jnp.float32)
            sq = wide * wide
            for j in range(piece // HD):
                squares = squares + sq[:, j * HD:(j + 1) * HD]
            scaled = (wide * gain[pl.ds(half * local + at, piece)].astype(jnp.float32).reshape(1, piece)).astype(jnp.bfloat16)
            acc = acc + jnp.dot(scaled, w_buf[slot], preferred_element_type=jnp.float32)
        total = jnp.sum(squares, axis=1, keepdims=True)
        acc = acc * lax.rsqrt(total / full + epsilon)
        for i in range(many):
            s = first + i
            living = position < lengths[s]
            for col in range(0, acc.shape[1], 2 * HD):
                key = acc[i * rows:(i + 1) * rows, col:col + HD]
                value = acc[i * rows:(i + 1) * rows, col + HD:col + 2 * HD]
                turned = key * cosine + pltpu.roll(key, HD // 2, 1) * sine
                buf[me, s, :, col:col + HD] = jnp.where(living, turned, 0.0).astype(jnp.bfloat16)
                buf[me, s, :, col + HD:col + 2 * HD] = jnp.where(living, value, 0.0).astype(jnp.bfloat16)

    project(0, 1)
    if halves:
        for u in range(halves):
            send_own(u)
    for s in range(1, seqs):
        project(s, 1)
        for u in range(s * halves, (s + 1) * halves):
            send_own(u)
    if not halves:
        send_own(0)

    if extra:
        side_copy(0, 0, 0, False).wait_recv()

        @pl.when(has_up)
        def _():
            up_send(0, count).start()

        @pl.when(has_down)
        def _():
            down_send(0, count).start()

    for step in range(1, n):
        id_landed(step).wait_recv()
    to_scalar = pltpu.make_async_copy(table_all, table_s, t_sem)
    to_scalar.start()
    to_scalar.wait()

    def look(dev, found):
        for s in range(seqs):
            page = table_s[dev, 0, s]
            found = tuple(
                jnp.where(page == me * SLOTS + j, dev * seqs + s, f) for j, f in enumerate(found)
            )
        return found

    found = lax.fori_loop(0, n, look, (jnp.int32(-1),) * SLOTS)

    for k in range(depth - 1):
        for u in range(stride):
            sideways = across == 2 and 0 < u < count

            @pl.when(z - 1 - k >= 0)
            def _():
                up_recv(k, u).wait_recv()
                if k + 1 < depth - 1:
                    @pl.when(has_up)
                    def _():
                        up_send(k + 1, u).start()
                if sideways:
                    side_copy(-(k + 1), u, up_base(k), True).start()

            @pl.when(z + 1 + k < depth)
            def _():
                down_recv(k, u).wait_recv()
                if k + 1 < depth - 1:
                    @pl.when(has_down)
                    def _():
                        down_send(k + 1, u).start()
                if sideways:
                    side_copy(k + 1, u, down_base(k), True).start()

    if across == 2:
        for u in range(1, count):
            side_copy(0, u, 0, False).wait_recv()
        for k in range(depth - 1):
            for u in range(1, count):
                @pl.when(z - 1 - k >= 0)
                def _():
                    side_copy(-(k + 1), u, up_base(k), False).wait_recv()

                @pl.when(z + 1 + k < depth)
                def _():
                    side_copy(k + 1, u, down_base(k), False).wait_recv()

    for j in range(SLOTS):
        index = jnp.maximum(found[j], 0)
        rows_j = buf[index // seqs, index % seqs]
        out[j] = jnp.where(found[j] >= 0, rows_j, jnp.zeros_like(rows_j))

    for s in range(seqs):
        for c in peer_copies[s]:
            c.wait_send()
    for step in range(1, n):
        id_copy(step).wait_send()
    for k in range(depth - 1):
        for u in range(stride):
            @pl.when(has_up & (z - k >= 0))
            def _():
                up_send(k, u).wait_send()

            @pl.when(has_down & (z + k < depth))
            def _():
                down_send(k, u).wait_send()
    if across == 2:
        for u in range(count):
            side_copy(0, u, 0, True).wait_send()
        for k in range(depth - 1):
            for u in range(1, count):
                @pl.when(z - 1 - k >= 0)
                def _():
                    side_copy(-(k + 1), u, up_base(k), True).wait_send()

                @pl.when(z + 1 + k < depth)
                def _():
                    side_copy(k + 1, u, down_base(k), True).wait_send()


def solution(mesh):
    n = mesh.shape["seq"]
    across = 2 if mesh.shape["group"] * 2 == PLANE and n % 2 == 0 else 1
    depth = n // across
    halves = 2 if across == 2 else 0

    def per_device(hidden, norm_gain, w_kv, lengths, page_table):
        seqs, rows, local = hidden.shape
        full, width = w_kv.shape
        assert rows == BLOCK and page_table.shape == (seqs, 1)
        piece = full // PIECES
        half_dim = HD // 2
        inv_freq = np.power(np.float64(rope_base), -2.0 * np.arange(half_dim) / HD)
        freq = jnp.asarray(np.tile(inv_freq, 2)[None, :].astype(np.float32))
        count = seqs * halves if halves else 1
        stride = count + (1 if across == 2 else 0)
        z_sems = pltpu.SemaphoreType.DMA((max(1, (depth - 1) * stride),))
        y_sems = pltpu.SemaphoreType.DMA((count * (2 * depth - 1) if across == 2 else 1,))
        vmem = pl.BlockSpec(memory_space=pltpu.VMEM)
        hbm = pl.BlockSpec(memory_space=pltpu.HBM)
        smem = pl.BlockSpec(memory_space=pltpu.SMEM)
        return pl.pallas_call(
            functools.partial(kernel, depth, across, halves),
            out_shape=pltpu.VMEM((SLOTS, BLOCK, width), jnp.bfloat16),
            in_specs=[hbm, vmem, hbm, smem, smem, vmem],
            out_specs=vmem,
            scratch_shapes=[
                pltpu.VMEM((seqs, rows, local), jnp.bfloat16),
                pltpu.VMEM((seqs, rows, local), jnp.bfloat16),
                pltpu.VMEM((PIECES, piece, width), jnp.bfloat16),
                pltpu.VMEM((n, seqs, rows, width), jnp.bfloat16),
                pltpu.VMEM((1, HD), jnp.int32),
                pltpu.VMEM((n, 1, HD), jnp.int32),
                pltpu.SMEM((n, 1, HD), jnp.int32),
                pltpu.SemaphoreType.DMA((seqs,)),
                pltpu.SemaphoreType.DMA((seqs * PIECES // 2,)),
                pltpu.SemaphoreType.DMA((seqs * PIECES // 2,)),
                pltpu.SemaphoreType.DMA((PIECES,)),
                pltpu.SemaphoreType.DMA((n - 1,)),
                pltpu.SemaphoreType.DMA((n - 1,)),
                pltpu.SemaphoreType.DMA,
                z_sems, z_sems, z_sems, z_sems, y_sems, y_sems,
            ],
            compiler_params=pltpu.CompilerParams(collective_id=0, has_side_effects=True, vmem_limit_bytes=63 * 1000 * 1024),
        )(hidden, norm_gain, w_kv, lengths, page_table.reshape(seqs), freq)

    return jax.shard_map(
        per_device,
        mesh=mesh,
        in_specs=(P("group", "seq", "tensor"), P(), P(None, "tensor"), P("group"), P("group", "seq")),
        out_specs=P(("group", "seq"), None, "tensor"),
        check_vma=False,
    )
```

```python
import functools

import jax
import jax.numpy as jnp
import numpy as np
from jax import lax
from jax.experimental import pallas as pl
from jax.experimental.pallas import tpu as pltpu
from jax.sharding import PartitionSpec as P

HD = 128
BLOCK = 128
SLOTS = 8
PIECES = 8
PLANE = 4

epsilon = 1e-05
rope_base = 500000.0
MESH = pl.DeviceIdType.MESH


def kernel(
    depth, across, slots,
    hidden, gain_hbm, w_kv, lengths_hbm, table_hbm, freq_hbm,
    out,
    h_own, h_peer, w_buf, buf, cross, gain, freq, lengths, table, table_all, table_s,
    h_sem, hs_sem, hr_sem, w_sem, in_sem, is_sem, ir_sem, t_sem,
    us_sem, ur_sem, ds_sem, dr_sem, ys_sem, yr_sem,
):
    n = depth * across
    seqs, rows, local = h_own.shape
    piece = w_buf.shape[1]
    per_half = PIECES // 2
    full = 2 * local
    me = lax.axis_index("seq")
    side = lax.axis_index("tensor")
    z = me // across
    y = me % across
    y_peer = z * across + (across - 1 - y)
    has_up = z + 1 < depth
    has_down = z >= 1
    pair = across == 2

    own_copies = [pltpu.make_async_copy(hidden.at[s], h_own.at[s], h_sem.at[s]) for s in range(seqs)]

    def w_copy(slot):
        half = side if slot < per_half else 1 - side
        index = half * per_half + slot % per_half
        return pltpu.make_async_copy(
            w_kv.at[pl.ds(index * piece, piece), :], w_buf.at[slot], w_sem.at[slot]
        )

    w_copies = [w_copy(i) for i in range(PIECES)]
    own_copies[0].start()
    for c in w_copies[:per_half]:
        c.start()
    smalls = [
        pltpu.make_async_copy(src, dst, in_sem.at[i])
        for i, (src, dst) in enumerate(
            [(table_hbm, table), (freq_hbm, freq), (gain_hbm, gain), (lengths_hbm, lengths)]
        )
    ]
    for c in smalls:
        c.start()

    barrier = pltpu.get_barrier_semaphore()

    def greet(device):
        pl.semaphore_signal(barrier, inc=1, device_id=device, device_id_type=MESH)

    greet({"tensor": 1 - side})
    if pair:
        greet({"seq": y_peer})

    @pl.when(has_up)
    def _():
        greet({"seq": me + across})

    @pl.when(has_down)
    def _():
        greet({"seq": me - across})

    pl.semaphore_wait(barrier, across + has_up.astype(jnp.int32) + has_down.astype(jnp.int32))

    def peer_copy(s, part):
        cut = pl.ds(part * piece, piece)
        i = s * per_half + part
        return pltpu.make_async_remote_copy(
            src_ref=hidden.at[s, :, cut], dst_ref=h_peer.at[s, :, cut],
            send_sem=hs_sem.at[i], recv_sem=hr_sem.at[i],
            device_id={"tensor": 1 - side}, device_id_type=MESH,
        )

    peer_copies = [[peer_copy(s, part) for part in range(per_half)] for s in range(seqs)]
    for c in peer_copies[0]:
        c.start()
    for c in w_copies[per_half:]:
        c.start()
    for s in range(1, seqs):
        own_copies[s].start()
        for c in peer_copies[s]:
            c.start()

    smalls[0].wait()
    id_lane = lax.broadcasted_iota(jnp.int32, (1, HD), 1)
    ids = jnp.full((1, HD), -1, jnp.int32)
    for s in range(seqs):
        ids = jnp.where(id_lane == s, table[s], ids)
    table_all[y, z] = ids
    smalls[1].wait()
    position = me * rows + lax.broadcasted_iota(jnp.int32, (rows, 1), 0)
    angle = position.astype(jnp.float32) * freq[...]
    cosine = jnp.cos(angle)
    lane = lax.broadcasted_iota(jnp.int32, (rows, HD), 1)
    sine = jnp.where(lane < HD // 2, -1.0, 1.0) * jnp.sin(angle)

    def send(src, dst, ssem, rsem, dev):
        return pltpu.make_async_remote_copy(
            src_ref=src, dst_ref=dst, send_sem=ssem, recv_sem=rsem,
            device_id={"seq": dev}, device_id_type=MESH,
        )

    part = rows // 2
    tail = (seqs - 1, 0)
    if pair:
        units = [(s, h) for s in range(seqs) for h in range(2) if (s, h) != tail] + [tail]
    else:
        units = [None]
    stride = len(units) + 1

    def half(block, h):
        return buf.at[block, pl.ds(h * part, part), :]

    def own_unit(dev, i):
        if not pair:
            return buf.at[pl.ds(dev * seqs, seqs)]
        return half(dev * seqs + units[i][0], units[i][1])

    def extra_unit(zz):
        return half((zz * across + across - 1 - y) * seqs + tail[0], tail[1])

    def up(ref, k, i, dev):
        return send(ref, ref, us_sem.at[k * stride + i], ur_sem.at[k * stride + i], dev)

    def down(ref, k, i, dev):
        return send(ref, ref, ds_sem.at[k * stride + i], dr_sem.at[k * stride + i], dev)

    def id_up(zz, k, dev):
        ref = table_all.at[y, zz]
        return send(ref, ref, is_sem.at[k], ir_sem.at[k], dev)

    def id_down(zz, k, dev):
        ref = table_all.at[y, zz]
        return send(ref, ref, is_sem.at[depth + k], ir_sem.at[depth + k], dev)

    def id_side(yy):
        ref = table_all.at[yy]
        return send(ref, ref, is_sem.at[2 * depth], ir_sem.at[2 * depth], y_peer)

    def tail_side(dev):
        ref = half(dev * seqs + tail[0], tail[1])
        return send(ref, ref, ys_sem.at[2 * slots], yr_sem.at[2 * slots], y_peer)

    def cross_send(j, h):
        cut = pl.ds(h * part, part)
        return send(
            cross.at[j, cut, :], buf.at[n * seqs + j, cut, :],
            ys_sem.at[2 * j + h], yr_sem.at[2 * j + h], y_peer,
        )

    def id_scalar(yy, zz, i):
        return pltpu.make_async_copy(table_all.at[yy, zz], table_s.at[yy, zz], t_sem.at[i])

    def send_own(i):
        @pl.when(has_down)
        def _():
            down(own_unit(me, i), 0, i, me - across).start()

        @pl.when(has_up)
        def _():
            up(own_unit(me, i), 0, i, me + across).start()

    def send_ids():
        @pl.when(has_down)
        def _():
            id_down(z, 0, me - across).start()

        @pl.when(has_up)
        def _():
            id_up(z, 0, me + across).start()

    def project(s):
        acc = jnp.zeros((rows, w_buf.shape[2]), jnp.float32)
        squares = jnp.zeros((rows, HD), jnp.float32)
        own_copies[s].wait()
        for slot in range(PIECES):
            if slot >= per_half:
                peer_copies[s][slot - per_half].wait_recv()
            if s == 0:
                w_copies[slot].wait()
            src = h_own if slot < per_half else h_peer
            half_of = side if slot < per_half else 1 - side
            at = (slot % per_half) * piece
            raw = src[s, :, pl.ds(at, piece)]
            wide = raw.astype(jnp.float32)
            sq = wide * wide
            for j in range(piece // HD):
                squares = squares + sq[:, j * HD:(j + 1) * HD]
            scaled = (wide * gain[pl.ds(half_of * local + at, piece)].astype(jnp.float32).reshape(1, piece)).astype(jnp.bfloat16)
            acc = acc + jnp.dot(scaled, w_buf[slot], preferred_element_type=jnp.float32)
        total = jnp.sum(squares, axis=1, keepdims=True)
        acc = acc * lax.rsqrt(total / full + epsilon)
        living = position < lengths[s]
        for col in range(0, acc.shape[1], 2 * HD):
            key = acc[:, col:col + HD]
            value = acc[:, col + HD:col + 2 * HD]
            turned = key * cosine + pltpu.roll(key, HD // 2, 1) * sine
            buf[me * seqs + s, :, col:col + HD] = jnp.where(living, turned, 0.0).astype(jnp.bfloat16)
            buf[me * seqs + s, :, col + HD:col + 2 * HD] = jnp.where(living, value, 0.0).astype(jnp.bfloat16)

    smalls[2].wait()
    smalls[3].wait()
    at_edge = (z == 0) | (z == depth - 1)
    for s in range(seqs):
        project(s)
        if s == 0:
            send_ids()
        if pair:
            if s == tail[0]:
                @pl.when(at_edge)
                def _():
                    tail_side(me).start()
            for i, (us, _) in enumerate(units):
                if us == s:
                    send_own(i)
    if not pair:
        send_own(0)
    own_scalar = id_scalar(y, z, 2 * depth)
    own_scalar.start()

    if pair:
        @pl.when(at_edge)
        def _():
            tail_side(y_peer).wait_recv()

        @pl.when(z == 0)
        def _():
            up(extra_unit(0), 0, stride - 1, me + across).start()

        @pl.when(z == depth - 1)
        def _():
            down(extra_unit(depth - 1), 0, stride - 1, me - across).start()

    own_scalar.wait()

    if not pair:
        for k in range(depth - 1):
            @pl.when(z - 1 - k >= 0)
            def _():
                id_up(z - 1 - k, k, me - across).wait_recv()
                if k + 1 < depth - 1:
                    @pl.when(has_up)
                    def _():
                        id_up(z - 1 - k, k + 1, me + across).start()
                up(own_unit(me - (k + 1), 0), k, 0, me - across).wait_recv()
                if k + 1 < depth - 1:
                    @pl.when(has_up)
                    def _():
                        up(own_unit(me - (k + 1), 0), k + 1, 0, me + across).start()

            @pl.when(z + 1 + k < depth)
            def _():
                id_down(z + 1 + k, k, me + across).wait_recv()
                if k + 1 < depth - 1:
                    @pl.when(has_down)
                    def _():
                        id_down(z + 1 + k, k + 1, me - across).start()
                down(own_unit(me + (k + 1), 0), k, 0, me + across).wait_recv()
                if k + 1 < depth - 1:
                    @pl.when(has_down)
                    def _():
                        down(own_unit(me + (k + 1), 0), k + 1, 0, me - across).start()

        to_scalar = pltpu.make_async_copy(table_all, table_s, t_sem.at[0])
        to_scalar.start()
        to_scalar.wait()

        def look(dev, found):
            for s in range(seqs):
                page = table_s[0, dev, 0, s]
                found = tuple(
                    jnp.where(page == me * SLOTS + j, dev * seqs + s, f) for j, f in enumerate(found)
                )
            return found

        found = lax.fori_loop(0, n, look, (jnp.int32(-1),) * SLOTS)
        where_is = [found, found]
    else:
        total = seqs * depth
        near = jnp.minimum(z, depth - 1 - z)
        below_far = z > depth - 1 - z
        first_pop = [total - 1 - slots, total - slots]

        def arrival(a):
            if a < seqs:
                return z, jnp.int32(a), z >= depth, jnp.int32(0)
            i = a - seqs
            both = i < near * 2 * seqs
            rest = i - near * 2 * seqs
            k = jnp.where(both, i // (2 * seqs), near + rest // seqs)
            s = jnp.where(both, (i % (2 * seqs)) // 2, rest % seqs)
            below = (both & (i % 2 == 0)) | (jnp.logical_not(both) & below_far)
            zz = jnp.where(below, z - 1 - k, z + 1 + k)
            return zz, s, below, k

        arrivals = [arrival(a) for a in range(total)]

        def is_tail(a):
            zz, s, _, _ = arrivals[a]
            return ((zz == 0) | (zz == depth - 1)) & (s == tail[0])

        def queue(lane_of, a, target, last, places):
            zz, s, _, _ = arrivals[a]
            page = table_s[lane_of, zz, 0, s]
            wanted = (page >= target * SLOTS) & (page < target * SLOTS + SLOTS)
            for h in range(2):
                goes = wanted & jnp.logical_not(is_tail(a)) if h == tail[1] else wanted
                place = jnp.maximum(last[h] + 1, max(a - first_pop[h], 0))
                places[h].append(jnp.where(goes, place, -1))
                last[h] = jnp.where(goes, place, last[h])

        def pop(h, a, places):
            j = a - first_pop[h]
            if j < 0 or j >= slots:
                return
            cut = pl.ds(h * part, part)
            content = None
            for c in range(j, a + 1):
                zz, s, _, _ = arrivals[c]
                rows_c = buf[(zz * across + y) * seqs + s, cut, :]
                content = rows_c if content is None else jnp.where(places[h][c] == j, rows_c, content)
            cross[j, cut, :] = content
            cross_send(j, h).start()

        def relay(a, h):
            zz, s, below, k = arrivals[a]
            ref = half((zz * across + y) * seqs + s, h)
            last_s = s == tail[0]
            i = jnp.where(last_s, 2 * seqs - 1 if h == tail[1] else 2 * seqs - 2, 2 * s + h)

            @pl.when(below)
            def _():
                up(ref, k, i, me - across).wait_recv()

                @pl.when(has_up)
                def _():
                    up(ref, k + 1, i, me + across).start()

            @pl.when(jnp.logical_not(below))
            def _():
                down(ref, k, i, me + across).wait_recv()

                @pl.when(has_down)
                def _():
                    down(ref, k + 1, i, me - across).start()

        def relay_id(a):
            zz, s, below, k = arrivals[a]

            @pl.when(below & (s == 0))
            def _():
                id_up(zz, k, me - across).wait_recv()

                @pl.when(has_up)
                def _():
                    id_up(zz, k + 1, me + across).start()

            @pl.when(jnp.logical_not(below) & (s == 0))
            def _():
                id_down(zz, k, me + across).wait_recv()

                @pl.when(has_down)
                def _():
                    id_down(zz, k + 1, me - across).start()

            @pl.when(s == 0)
            def _():
                id_scalar(y, zz, zz).start()

        def relay_extra(a):
            zz, s, below, k = arrivals[a]

            @pl.when(is_tail(a) & below)
            def _():
                up(extra_unit(zz), k, stride - 1, me - across).wait_recv()

                @pl.when(has_up)
                def _():
                    up(extra_unit(zz), k + 1, stride - 1, me + across).start()

            @pl.when(is_tail(a) & jnp.logical_not(below))
            def _():
                down(extra_unit(zz), k, stride - 1, me + across).wait_recv()

                @pl.when(has_down)
                def _():
                    down(extra_unit(zz), k + 1, stride - 1, me - across).start()

        last = [jnp.int32(-1), jnp.int32(-1)]
        places = [[], []]
        for a in range(seqs):
            queue(y, a, y_peer, last, places)
        for a in range(seqs, total):
            zz, s, _, _ = arrivals[a]
            relay_id(a)
            order = (1 - tail[1], tail[1]) if a == total - 1 else (0, 1)
            relay(a, order[0])

            @pl.when(s == 0)
            def _():
                id_scalar(y, zz, zz).wait()

            queue(y, a, y_peer, last, places)
            if a == total - seqs:
                id_side(y).start()
            if a == total - 2:
                pop(order[0], a, places)
                relay(a, order[1])
                pop(order[1], a, places)
                relay_extra(a)
                id_side(1 - y).wait_recv()
                rest = pltpu.make_async_copy(table_all.at[1 - y], table_s.at[1 - y], t_sem.at[2 * depth + 1])
                rest.start()
                rest.wait()
                continue
            if a == total - 1:
                found = [[jnp.int32(-1)] * SLOTS for _ in range(2)]
                peer_last = [jnp.int32(-1), jnp.int32(-1)]
                peer_places = [[], []]
                for c in range(total):
                    cz, cs, _, _ = arrivals[c]
                    queue(1 - y, c, me, peer_last, peer_places)
                    mine = table_s[y, cz, 0, cs] - me * SLOTS
                    theirs = table_s[1 - y, cz, 0, cs] - me * SLOTS
                    here = (cz * across + y) * seqs + cs
                    there = (cz * across + 1 - y) * seqs + cs
                    for h in range(2):
                        place = n * seqs + peer_places[h][c]
                        if h == tail[1]:
                            place = jnp.where(is_tail(c), there, place)
                        found[h] = [
                            jnp.where(mine == j, here, jnp.where(theirs == j, place, f))
                            for j, f in enumerate(found[h])
                        ]
                where_is = found
            pop(order[0], a, places)
            relay(a, order[1])
            pop(order[1], a, places)
            relay_extra(a)
        for j in range(slots):
            for h in range(2):
                cross_send(j, h).wait_recv()

    for h in range(2):
        cut = pl.ds(h * part, part)
        for j in range(SLOTS):
            index = where_is[h][j]
            rows_j = buf[jnp.maximum(index, 0), cut, :]
            out[j, cut, :] = jnp.where(index >= 0, rows_j, jnp.zeros_like(rows_j))

    for s in range(seqs):
        for c in peer_copies[s]:
            c.wait_send()
    for k in range(depth - 1):
        @pl.when(has_up & (z - k >= 0))
        def _():
            id_up(z - k, k, me + across).wait_send()
            for i in range(len(units)):
                up(own_unit(me - k * across, i), k, i, me + across).wait_send()

        @pl.when(has_down & (z + k < depth))
        def _():
            id_down(z + k, k, me - across).wait_send()
            for i in range(len(units)):
                down(own_unit(me + k * across, i), k, i, me - across).wait_send()
    if pair:
        @pl.when(has_up)
        def _():
            up(extra_unit(0), z, stride - 1, me + across).wait_send()

        @pl.when(has_down)
        def _():
            down(extra_unit(depth - 1), depth - 1 - z, stride - 1, me - across).wait_send()

        @pl.when(at_edge)
        def _():
            tail_side(me).wait_send()

        id_side(y).wait_send()
        for j in range(slots):
            for h in range(2):
                cross_send(j, h).wait_send()


def solution(mesh):
    n = mesh.shape["seq"]

    def per_device(hidden, norm_gain, w_kv, lengths, page_table):
        seqs, rows, local = hidden.shape
        full, width = w_kv.shape
        assert rows == BLOCK and page_table.shape == (seqs, 1)
        wide = mesh.shape["group"] * 2 == PLANE and n % 2 == 0 and seqs * (n // 2) > SLOTS
        across = 2 if wide else 1
        depth = n // across
        slots = SLOTS if wide else 0
        piece = full // PIECES
        half_dim = HD // 2
        inv_freq = np.power(np.float64(rope_base), -2.0 * np.arange(half_dim) / HD)
        freq = jnp.asarray(np.tile(inv_freq, 2)[None, :].astype(np.float32))
        stride = (2 * seqs if wide else 1) + 1
        z_sems = pltpu.SemaphoreType.DMA((max(1, (depth - 1) * stride),))
        y_sems = pltpu.SemaphoreType.DMA((2 * slots + 1,))
        vmem = pl.BlockSpec(memory_space=pltpu.VMEM)
        hbm = pl.BlockSpec(memory_space=pltpu.HBM)
        return pl.pallas_call(
            functools.partial(kernel, depth, across, slots),
            out_shape=pltpu.VMEM((SLOTS, BLOCK, width), jnp.bfloat16),
            in_specs=[hbm] * 6,
            out_specs=vmem,
            scratch_shapes=[
                pltpu.VMEM((seqs, rows, local), jnp.bfloat16),
                pltpu.VMEM((seqs, rows, local), jnp.bfloat16),
                pltpu.VMEM((PIECES, piece, width), jnp.bfloat16),
                pltpu.VMEM((n * seqs + slots, rows, width), jnp.bfloat16),
                pltpu.VMEM((max(1, slots), rows, width), jnp.bfloat16),
                pltpu.VMEM((full,), jnp.bfloat16),
                pltpu.VMEM((1, HD), jnp.float32),
                pltpu.SMEM((seqs,), jnp.int32),
                pltpu.SMEM((seqs,), jnp.int32),
                pltpu.VMEM((across, depth, 1, HD), jnp.int32),
                pltpu.SMEM((across, depth, 1, HD), jnp.int32),
                pltpu.SemaphoreType.DMA((seqs,)),
                pltpu.SemaphoreType.DMA((seqs * PIECES // 2,)),
                pltpu.SemaphoreType.DMA((seqs * PIECES // 2,)),
                pltpu.SemaphoreType.DMA((PIECES,)),
                pltpu.SemaphoreType.DMA((4,)),
                pltpu.SemaphoreType.DMA((2 * depth + 1,)),
                pltpu.SemaphoreType.DMA((2 * depth + 1,)),
                pltpu.SemaphoreType.DMA((2 * depth + 2,)),
                z_sems, z_sems, z_sems, z_sems, y_sems, y_sems,
            ],
            compiler_params=pltpu.CompilerParams(collective_id=0, has_side_effects=True, vmem_limit_bytes=63 * 1000 * 1024),
        )(hidden, norm_gain, w_kv, lengths, page_table.reshape(seqs), freq)

    return jax.shard_map(
        per_device,
        mesh=mesh,
        in_specs=(P("group", "seq", "tensor"), P(), P(None, "tensor"), P("group"), P("group", "seq")),
        out_specs=P(("group", "seq"), None, "tensor"),
        check_vma=False,
    )
```

```python
import functools

import jax
import jax.numpy as jnp
import numpy as np
from jax import lax
from jax.experimental import pallas as pl
from jax.experimental.pallas import tpu as pltpu
from jax.sharding import PartitionSpec as P

HD = 128
BLOCK = 128
SLOTS = 8
PIECES = 8
PLANE = 4

epsilon = 1e-05
rope_base = 500000.0
MESH = pl.DeviceIdType.MESH


def kernel(
    depth, across, slots,
    hidden, gain_hbm, w_kv, lengths_hbm, table_hbm, freq_hbm,
    out,
    h_own, h_peer, w_buf, buf, cross, gain, freq, lengths, table, table_all, table_s,
    h_sem, hs_sem, hr_sem, w_sem, in_sem, is_sem, ir_sem, t_sem,
    us_sem, ur_sem, ds_sem, dr_sem, ys_sem, yr_sem, in_up, in_side,
):
    n = depth * across
    seqs, rows, local = h_own.shape
    piece = w_buf.shape[1]
    per_half = PIECES // 2
    full = 2 * local
    me = lax.axis_index("seq")
    side = lax.axis_index("tensor")
    z = me // across
    y = me % across
    y_peer = z * across + (across - 1 - y)
    has_up = z + 1 < depth
    has_down = z >= 1
    pair = across == 2

    own_copies = [pltpu.make_async_copy(hidden.at[s], h_own.at[s], h_sem.at[s]) for s in range(seqs)]

    def w_copy(slot):
        half = side if slot < per_half else 1 - side
        index = half * per_half + slot % per_half
        return pltpu.make_async_copy(
            w_kv.at[pl.ds(index * piece, piece), :], w_buf.at[slot], w_sem.at[slot]
        )

    w_copies = [w_copy(i) for i in range(PIECES)]
    own_copies[0].start()
    for c in w_copies[:per_half]:
        c.start()
    smalls = [
        pltpu.make_async_copy(src, dst, in_sem.at[i])
        for i, (src, dst) in enumerate(
            [(table_hbm, table), (freq_hbm, freq), (gain_hbm, gain), (lengths_hbm, lengths)]
        )
    ]
    for c in smalls:
        c.start()

    barrier = pltpu.get_barrier_semaphore()

    def greet(device):
        pl.semaphore_signal(barrier, inc=1, device_id=device, device_id_type=MESH)

    greet({"tensor": 1 - side})

    @pl.when(has_up)
    def _():
        greet({"seq": me + across})

    expected = 1 + has_down.astype(jnp.int32)
    if pair:
        @pl.when(y == 0)
        def _():
            greet({"seq": y_peer})

        expected = expected + y
    pl.semaphore_wait(barrier, expected)

    def peer_copy(s, part):
        cut = pl.ds(part * piece, piece)
        i = s * per_half + part
        return pltpu.make_async_remote_copy(
            src_ref=hidden.at[s, :, cut], dst_ref=h_peer.at[s, :, cut],
            send_sem=hs_sem.at[i], recv_sem=hr_sem.at[i],
            device_id={"tensor": 1 - side}, device_id_type=MESH,
        )

    peer_copies = [[peer_copy(s, part) for part in range(per_half)] for s in range(seqs)]
    for c in peer_copies[0]:
        c.start()
    for c in w_copies[per_half:]:
        c.start()
    for s in range(1, seqs):
        own_copies[s].start()
        for c in peer_copies[s]:
            c.start()

    @pl.when(has_down)
    def _():
        pl.semaphore_signal(in_up, inc=1, device_id={"seq": me - across}, device_id_type=MESH)

    if pair:
        @pl.when(y == 1)
        def _():
            pl.semaphore_signal(in_side, inc=1, device_id={"seq": y_peer}, device_id_type=MESH)

    smalls[0].wait()
    id_lane = lax.broadcasted_iota(jnp.int32, (1, HD), 1)
    ids = jnp.full((1, HD), -1, jnp.int32)
    for s in range(seqs):
        ids = jnp.where(id_lane == s, table[s], ids)
    table_all[y, z] = ids
    smalls[1].wait()
    position = me * rows + lax.broadcasted_iota(jnp.int32, (rows, 1), 0)
    angle = position.astype(jnp.float32) * freq[...]
    cosine = jnp.cos(angle)
    lane = lax.broadcasted_iota(jnp.int32, (rows, HD), 1)
    sine = jnp.where(lane < HD // 2, -1.0, 1.0) * jnp.sin(angle)

    def send(src, dst, ssem, rsem, dev):
        return pltpu.make_async_remote_copy(
            src_ref=src, dst_ref=dst, send_sem=ssem, recv_sem=rsem,
            device_id={"seq": dev}, device_id_type=MESH,
        )

    part = rows // 2
    quarter = rows // 4
    tail = seqs - 1
    pieces = [(part, quarter), (part + quarter, quarter), (0, part)]
    if pair:
        units = [(s, lo, part) for s in range(tail) for lo in (0, part)] + [(tail, lo, size) for lo, size in pieces]
    else:
        units = [None]
    stride = len(units) + 1

    def strip(block, lo, size):
        return buf.at[block, pl.ds(lo, size), :]

    def own_unit(dev, i):
        if not pair:
            return buf.at[pl.ds(dev * seqs, seqs)]
        return strip(dev * seqs + units[i][0], units[i][1], units[i][2])

    def extra_unit(zz):
        return strip((zz * across + across - 1 - y) * seqs + tail, 0, part)

    def up(ref, k, i, dev):
        return send(ref, ref, us_sem.at[k * stride + i], ur_sem.at[k * stride + i], dev)

    def down(ref, k, i, dev):
        return send(ref, ref, ds_sem.at[k * stride + i], dr_sem.at[k * stride + i], dev)

    def id_up(zz, k, dev):
        ref = table_all.at[y, zz]
        return send(ref, ref, is_sem.at[k], ir_sem.at[k], dev)

    def id_down(zz, k, dev):
        ref = table_all.at[y, zz]
        return send(ref, ref, is_sem.at[depth + k], ir_sem.at[depth + k], dev)

    def id_side(yy):
        ref = table_all.at[yy]
        return send(ref, ref, is_sem.at[2 * depth], ir_sem.at[2 * depth], y_peer)

    def tail_side(dev):
        ref = strip(dev * seqs + tail, 0, part)
        return send(ref, ref, ys_sem.at[3 * slots], yr_sem.at[3 * slots], y_peer)

    def cross_pieces(h, j):
        if h == 0:
            return [(0, part)]
        if j < slots - 1:
            return [(part, part)]
        return [(part, quarter), (part + quarter, quarter)]

    def cross_send(j, lo, size):
        i = 3 * j + (0 if lo == 0 else 1 if lo == part else 2)
        cut = pl.ds(lo, size)
        return send(
            cross.at[j, cut, :], buf.at[n * seqs + j, cut, :], ys_sem.at[i], yr_sem.at[i], y_peer,
        )

    all_cross = [(j, lo, size) for j in range(slots) for h in range(2) for lo, size in cross_pieces(h, j)]

    def id_scalar(yy, zz, i):
        return pltpu.make_async_copy(table_all.at[yy, zz], table_s.at[yy, zz], t_sem.at[i])

    def send_own(i):
        @pl.when(has_down)
        def _():
            down(own_unit(me, i), 0, i, me - across).start()

        @pl.when(has_up)
        def _():
            up(own_unit(me, i), 0, i, me + across).start()

    def send_ids():
        @pl.when(has_down)
        def _():
            id_down(z, 0, me - across).start()

        @pl.when(has_up)
        def _():
            pl.semaphore_wait(in_up, 1)
            id_up(z, 0, me + across).start()

    def project(s):
        acc = jnp.zeros((rows, w_buf.shape[2]), jnp.float32)
        squares = jnp.zeros((rows, HD), jnp.float32)
        own_copies[s].wait()
        for slot in range(PIECES):
            if slot >= per_half:
                peer_copies[s][slot - per_half].wait_recv()
            if s == 0:
                w_copies[slot].wait()
            src = h_own if slot < per_half else h_peer
            half_of = side if slot < per_half else 1 - side
            at = (slot % per_half) * piece
            raw = src[s, :, pl.ds(at, piece)]
            wide = raw.astype(jnp.float32)
            sq = wide * wide
            for j in range(piece // HD):
                squares = squares + sq[:, j * HD:(j + 1) * HD]
            scaled = (wide * gain[pl.ds(half_of * local + at, piece)].astype(jnp.float32).reshape(1, piece)).astype(jnp.bfloat16)
            acc = acc + jnp.dot(scaled, w_buf[slot], preferred_element_type=jnp.float32)
        total = jnp.sum(squares, axis=1, keepdims=True)
        acc = acc * lax.rsqrt(total / full + epsilon)
        living = position < lengths[s]
        for col in range(0, acc.shape[1], 2 * HD):
            key = acc[:, col:col + HD]
            value = acc[:, col + HD:col + 2 * HD]
            turned = key * cosine + pltpu.roll(key, HD // 2, 1) * sine
            buf[me * seqs + s, :, col:col + HD] = jnp.where(living, turned, 0.0).astype(jnp.bfloat16)
            buf[me * seqs + s, :, col + HD:col + 2 * HD] = jnp.where(living, value, 0.0).astype(jnp.bfloat16)

    def settle(ks):
        for k in ks:
            @pl.when(has_up & (z - k >= 0))
            def _():
                id_up(z - k, k, me + across).wait_send()
                for i in range(len(units)):
                    up(own_unit(me - k * across, i), k, i, me + across).wait_send()

            @pl.when(has_down & (z + k < depth))
            def _():
                id_down(z + k, k, me - across).wait_send()
                for i in range(len(units)):
                    down(own_unit(me + k * across, i), k, i, me - across).wait_send()

    smalls[2].wait()
    smalls[3].wait()
    at_edge = (z == 0) | (z == depth - 1)
    for s in range(seqs):
        project(s)
        if s == 0:
            send_ids()
        if pair:
            if s == tail:
                @pl.when(y == 0)
                def _():
                    pl.semaphore_wait(in_side, 1)

                @pl.when(at_edge)
                def _():
                    tail_side(me).start()
            mine = [i for i, unit in enumerate(units) if unit[0] == s]
            if s < tail:
                for i in mine:
                    send_own(i)
            else:
                for when, order in ((at_edge, mine), (jnp.logical_not(at_edge), mine[-1:] + mine[:-1])):
                    @pl.when(when)
                    def _():
                        for i in order:
                            send_own(i)
    if not pair:
        send_own(0)
    for s in range(seqs):
        for c in peer_copies[s]:
            c.wait_send()
    own_scalar = id_scalar(y, z, 2 * depth)
    own_scalar.start()

    if pair:
        @pl.when(at_edge)
        def _():
            tail_side(y_peer).wait_recv()

        @pl.when(z == 0)
        def _():
            up(extra_unit(0), 0, stride - 1, me + across).start()

        @pl.when(z == depth - 1)
        def _():
            down(extra_unit(depth - 1), 0, stride - 1, me - across).start()

    own_scalar.wait()

    if not pair:
        for k in range(depth - 1):
            @pl.when(z - 1 - k >= 0)
            def _():
                id_up(z - 1 - k, k, me - across).wait_recv()
                if k + 1 < depth - 1:
                    @pl.when(has_up)
                    def _():
                        id_up(z - 1 - k, k + 1, me + across).start()
                up(own_unit(me - (k + 1), 0), k, 0, me - across).wait_recv()
                if k + 1 < depth - 1:
                    @pl.when(has_up)
                    def _():
                        up(own_unit(me - (k + 1), 0), k + 1, 0, me + across).start()

            @pl.when(z + 1 + k < depth)
            def _():
                id_down(z + 1 + k, k, me + across).wait_recv()
                if k + 1 < depth - 1:
                    @pl.when(has_down)
                    def _():
                        id_down(z + 1 + k, k + 1, me - across).start()
                down(own_unit(me + (k + 1), 0), k, 0, me + across).wait_recv()
                if k + 1 < depth - 1:
                    @pl.when(has_down)
                    def _():
                        down(own_unit(me + (k + 1), 0), k + 1, 0, me - across).start()

        to_scalar = pltpu.make_async_copy(table_all, table_s, t_sem.at[0])
        to_scalar.start()
        to_scalar.wait()

        def look(dev, found):
            for s in range(seqs):
                page = table_s[0, dev, 0, s]
                found = tuple(
                    jnp.where(page == me * SLOTS + j, dev * seqs + s, f) for j, f in enumerate(found)
                )
            return found

        found = lax.fori_loop(0, n, look, (jnp.int32(-1),) * SLOTS)
        where_is = [found, found]
    else:
        total = seqs * depth
        near = jnp.minimum(z, depth - 1 - z)
        below_far = z > depth - 1 - z
        first_pop = [total - 1 - slots, total - slots]

        def arrival(a):
            if a < seqs:
                return z, jnp.int32(a), z >= depth, jnp.int32(0)
            i = a - seqs
            both = i < near * 2 * seqs
            rest = i - near * 2 * seqs
            k = jnp.where(both, i // (2 * seqs), near + rest // seqs)
            s = jnp.where(both, (i % (2 * seqs)) // 2, rest % seqs)
            below = (both & (i % 2 == 0)) | (jnp.logical_not(both) & below_far)
            zz = jnp.where(below, z - 1 - k, z + 1 + k)
            return zz, s, below, k

        arrivals = [arrival(a) for a in range(total)]

        def is_tail(a):
            zz, s, _, _ = arrivals[a]
            return ((zz == 0) | (zz == depth - 1)) & (s == tail)

        def queue(lane_of, a, target, last, places):
            zz, s, _, _ = arrivals[a]
            page = table_s[lane_of, zz, 0, s]
            wanted = (page >= target * SLOTS) & (page < target * SLOTS + SLOTS)
            for h in range(2):
                goes = wanted & jnp.logical_not(is_tail(a)) if h == 0 else wanted
                place = jnp.maximum(last[h] + 1, max(a - first_pop[h], 0))
                places[h].append(jnp.where(goes, place, -1))
                last[h] = jnp.where(goes, place, last[h])

        def pop(h, a, places, cuts=None):
            j = a - first_pop[h]
            if j < 0 or j >= slots:
                return
            for lo, size in cuts or cross_pieces(h, j):
                cut = pl.ds(lo, size)
                content = None
                for c in range(j, a + 1):
                    zz, s, _, _ = arrivals[c]
                    rows_c = buf[(zz * across + y) * seqs + s, cut, :]
                    content = rows_c if content is None else jnp.where(places[h][c] == j, rows_c, content)
                cross[j, cut, :] = content
                cross_send(j, lo, size).start()

        def relay(a, when, i, lo, size):
            zz, s, below, k = arrivals[a]
            ref = strip((zz * across + y) * seqs + s, lo, size)

            @pl.when(when & below)
            def _():
                up(ref, k, i, me - across).wait_recv()

                @pl.when(has_up)
                def _():
                    up(ref, k + 1, i, me + across).start()

            @pl.when(when & jnp.logical_not(below))
            def _():
                down(ref, k, i, me + across).wait_recv()

                @pl.when(has_down)
                def _():
                    down(ref, k + 1, i, me - across).start()

        def relay_id(a):
            zz, s, below, k = arrivals[a]

            @pl.when(below & (s == 0))
            def _():
                id_up(zz, k, me - across).wait_recv()

                @pl.when(has_up)
                def _():
                    id_up(zz, k + 1, me + across).start()

            @pl.when(jnp.logical_not(below) & (s == 0))
            def _():
                id_down(zz, k, me + across).wait_recv()

                @pl.when(has_down)
                def _():
                    id_down(zz, k + 1, me - across).start()

            @pl.when(s == 0)
            def _():
                id_scalar(y, zz, zz).start()

        def relay_extra(a):
            zz, s, below, k = arrivals[a]

            @pl.when(is_tail(a) & below)
            def _():
                up(extra_unit(zz), k, stride - 1, me - across).wait_recv()

                @pl.when(has_up)
                def _():
                    up(extra_unit(zz), k + 1, stride - 1, me + across).start()

            @pl.when(is_tail(a) & jnp.logical_not(below))
            def _():
                down(extra_unit(zz), k, stride - 1, me + across).wait_recv()

                @pl.when(has_down)
                def _():
                    down(extra_unit(zz), k + 1, stride - 1, me - across).start()

        last = [jnp.int32(-1), jnp.int32(-1)]
        places = [[], []]
        for a in range(seqs):
            queue(y, a, y_peer, last, places)
        for a in range(seqs, total):
            zz, s, _, _ = arrivals[a]
            relay_id(a)
            ending = a == total - 1
            if not ending:
                relay(a, s < tail, 2 * s, 0, part)
                relay(a, s == tail, stride - 2, 0, part)

            @pl.when(s == 0)
            def _():
                id_scalar(y, zz, zz).wait()

            queue(y, a, y_peer, last, places)
            if a == total - seqs:
                id_side(y).start()
            if not ending:
                pop(0, a, places)
                relay(a, s < tail, 2 * s + 1, part, part)
            for t, (lo, size) in enumerate(pieces):
                if ending or lo:
                    relay(a, s == tail, 2 * tail + t, lo, size)
                if ending:
                    pop(1 if lo else 0, a, places, [(lo, size)])
            if not ending:
                pop(1, a, places)
            relay_extra(a)
            if a == total - 2:
                id_side(1 - y).wait_recv()
                rest = pltpu.make_async_copy(table_all.at[1 - y], table_s.at[1 - y], t_sem.at[2 * depth + 1])
                rest.start()
                rest.wait()
                found = [[jnp.int32(-1)] * SLOTS for _ in range(2)]
                peer_last = [jnp.int32(-1), jnp.int32(-1)]
                peer_places = [[], []]
                for c in range(total):
                    cz, cs, _, _ = arrivals[c]
                    queue(1 - y, c, me, peer_last, peer_places)
                    mine = table_s[y, cz, 0, cs] - me * SLOTS
                    theirs = table_s[1 - y, cz, 0, cs] - me * SLOTS
                    here = (cz * across + y) * seqs + cs
                    there = (cz * across + 1 - y) * seqs + cs
                    for h in range(2):
                        place = n * seqs + peer_places[h][c]
                        if h == 0:
                            place = jnp.where(is_tail(c), there, place)
                        found[h] = [
                            jnp.where(mine == j, here, jnp.where(theirs == j, place, f))
                            for j, f in enumerate(found[h])
                        ]
                where_is = found
                settle(range(depth - 2))
        for piece_of in all_cross:
            cross_send(*piece_of).wait_recv()

    for h in range(2):
        cut = pl.ds(h * part, part)
        for j in range(SLOTS):
            index = where_is[h][j]
            rows_j = buf[jnp.maximum(index, 0), cut, :]
            out[j, cut, :] = jnp.where(index >= 0, rows_j, jnp.zeros_like(rows_j))

    settle(range(depth - 2, depth - 1) if pair else range(depth - 1))
    if pair:
        @pl.when(has_up)
        def _():
            up(extra_unit(0), z, stride - 1, me + across).wait_send()

        @pl.when(has_down)
        def _():
            down(extra_unit(depth - 1), depth - 1 - z, stride - 1, me - across).wait_send()

        @pl.when(at_edge)
        def _():
            tail_side(me).wait_send()

        id_side(y).wait_send()
        for piece_of in all_cross:
            cross_send(*piece_of).wait_send()


def solution(mesh):
    n = mesh.shape["seq"]

    def per_device(hidden, norm_gain, w_kv, lengths, page_table):
        seqs, rows, local = hidden.shape
        full, width = w_kv.shape
        assert rows == BLOCK and page_table.shape == (seqs, 1)
        wide = mesh.shape["group"] * 2 == PLANE and n % 2 == 0 and seqs * (n // 2) > SLOTS
        across = 2 if wide else 1
        depth = n // across
        slots = SLOTS if wide else 0
        piece = full // PIECES
        half_dim = HD // 2
        inv_freq = np.power(np.float64(rope_base), -2.0 * np.arange(half_dim) / HD)
        freq = jnp.asarray(np.tile(inv_freq, 2)[None, :].astype(np.float32))
        stride = (2 * seqs + 1 if wide else 1) + 1
        z_sems = pltpu.SemaphoreType.DMA((max(1, (depth - 1) * stride),))
        y_sems = pltpu.SemaphoreType.DMA((3 * slots + 1,))
        vmem = pl.BlockSpec(memory_space=pltpu.VMEM)
        hbm = pl.BlockSpec(memory_space=pltpu.HBM)
        return pl.pallas_call(
            functools.partial(kernel, depth, across, slots),
            out_shape=pltpu.VMEM((SLOTS, BLOCK, width), jnp.bfloat16),
            in_specs=[hbm] * 6,
            out_specs=vmem,
            scratch_shapes=[
                pltpu.VMEM((seqs, rows, local), jnp.bfloat16),
                pltpu.VMEM((seqs, rows, local), jnp.bfloat16),
                pltpu.VMEM((PIECES, piece, width), jnp.bfloat16),
                pltpu.VMEM((n * seqs + slots, rows, width), jnp.bfloat16),
                pltpu.VMEM((max(1, slots), rows, width), jnp.bfloat16),
                pltpu.VMEM((full,), jnp.bfloat16),
                pltpu.VMEM((1, HD), jnp.float32),
                pltpu.SMEM((seqs,), jnp.int32),
                pltpu.SMEM((seqs,), jnp.int32),
                pltpu.VMEM((across, depth, 1, HD), jnp.int32),
                pltpu.SMEM((across, depth, 1, HD), jnp.int32),
                pltpu.SemaphoreType.DMA((seqs,)),
                pltpu.SemaphoreType.DMA((seqs * PIECES // 2,)),
                pltpu.SemaphoreType.DMA((seqs * PIECES // 2,)),
                pltpu.SemaphoreType.DMA((PIECES,)),
                pltpu.SemaphoreType.DMA((4,)),
                pltpu.SemaphoreType.DMA((2 * depth + 1,)),
                pltpu.SemaphoreType.DMA((2 * depth + 1,)),
                pltpu.SemaphoreType.DMA((2 * depth + 2,)),
                z_sems, z_sems, z_sems, z_sems, y_sems, y_sems,
                pltpu.SemaphoreType.REGULAR,
                pltpu.SemaphoreType.REGULAR,
            ],
            compiler_params=pltpu.CompilerParams(collective_id=0, has_side_effects=True, vmem_limit_bytes=63 * 1000 * 1024),
        )(hidden, norm_gain, w_kv, lengths, page_table.reshape(seqs), freq)

    return jax.shard_map(
        per_device,
        mesh=mesh,
        in_specs=(P("group", "seq", "tensor"), P(), P(None, "tensor"), P("group"), P("group", "seq")),
        out_specs=P(("group", "seq"), None, "tensor"),
        check_vma=False,
    )
```

```python
import functools

import jax
import jax.numpy as jnp
import numpy as np
from jax import lax
from jax.experimental import pallas as pl
from jax.experimental.pallas import tpu as pltpu
from jax.sharding import PartitionSpec as P

HD = 128
BLOCK = 128
SLOTS = 8
PIECES = 8
PLANE = 4

epsilon = 1e-05
rope_base = 500000.0
MESH = pl.DeviceIdType.MESH


def kernel(
    depth, across, slots,
    hidden, gain_hbm, w_kv, lengths_hbm, table_hbm, freq_hbm,
    out,
    h_own, h_peer, w_buf, buf, cross, gain, freq, lengths, table, table_all, table_s,
    h_sem, hs_sem, hr_sem, w_sem, in_sem, is_sem, ir_sem, t_sem,
    us_sem, ur_sem, ds_sem, dr_sem, ys_sem, yr_sem, in_up, in_side,
):
    n = depth * across
    seqs, rows, local = h_own.shape
    piece = w_buf.shape[1]
    per_half = PIECES // 2
    full = 2 * local
    me = lax.axis_index("seq")
    side = lax.axis_index("tensor")
    z = me // across
    y = me % across
    y_peer = z * across + (across - 1 - y)
    has_up = z + 1 < depth
    has_down = z >= 1
    pair = across == 2
    twice = side == 0

    own_copies = [pltpu.make_async_copy(hidden.at[s], h_own.at[s], h_sem.at[s]) for s in range(seqs)]

    def w_copy(slot):
        half = side if slot < per_half else 1 - side
        index = half * per_half + slot % per_half
        return pltpu.make_async_copy(
            w_kv.at[pl.ds(index * piece, piece), :], w_buf.at[slot], w_sem.at[slot]
        )

    w_copies = [w_copy(i) for i in range(PIECES)]
    own_copies[0].start()
    for c in w_copies[:per_half]:
        c.start()
    smalls = [
        pltpu.make_async_copy(src, dst, in_sem.at[i])
        for i, (src, dst) in enumerate(
            [(table_hbm, table), (freq_hbm, freq), (gain_hbm, gain), (lengths_hbm, lengths)]
        )
    ]
    for c in smalls:
        c.start()

    barrier = pltpu.get_barrier_semaphore()

    def greet(device):
        pl.semaphore_signal(barrier, inc=1, device_id=device, device_id_type=MESH)

    greet({"tensor": 1 - side})

    @pl.when(has_up)
    def _():
        greet({"seq": me + across})

    expected = 1 + has_down.astype(jnp.int32)
    if pair:
        @pl.when(y == 0)
        def _():
            greet({"seq": y_peer})

        expected = expected + y
    pl.semaphore_wait(barrier, expected)

    def peer_copy(s, part):
        cut = pl.ds(part * piece, piece)
        i = s * per_half + part
        return pltpu.make_async_remote_copy(
            src_ref=hidden.at[s, :, cut], dst_ref=h_peer.at[s, :, cut],
            send_sem=hs_sem.at[i], recv_sem=hr_sem.at[i],
            device_id={"tensor": 1 - side}, device_id_type=MESH,
        )

    peer_copies = [[peer_copy(s, part) for part in range(per_half)] for s in range(seqs)]
    for c in peer_copies[0]:
        c.start()
    for c in w_copies[per_half:]:
        c.start()
    for s in range(1, seqs):
        own_copies[s].start()
        for c in peer_copies[s]:
            c.start()

    @pl.when(has_down)
    def _():
        pl.semaphore_signal(in_up, inc=1, device_id={"seq": me - across}, device_id_type=MESH)

    if pair:
        @pl.when(y == 1)
        def _():
            pl.semaphore_signal(in_side, inc=1, device_id={"seq": y_peer}, device_id_type=MESH)

    smalls[0].wait()
    id_lane = lax.broadcasted_iota(jnp.int32, (1, HD), 1)
    ids = jnp.full((1, HD), -1, jnp.int32)
    for s in range(seqs):
        ids = jnp.where(id_lane == s, table[s], ids)
    table_all[y, z] = ids
    smalls[1].wait()
    position = me * rows + lax.broadcasted_iota(jnp.int32, (rows, 1), 0)
    angle = position.astype(jnp.float32) * freq[...]
    cosine = jnp.cos(angle)
    lane = lax.broadcasted_iota(jnp.int32, (rows, HD), 1)
    sine = jnp.where(lane < HD // 2, -1.0, 1.0) * jnp.sin(angle)

    def send(src, dst, ssem, rsem, dev):
        return pltpu.make_async_remote_copy(
            src_ref=src, dst_ref=dst, send_sem=ssem, recv_sem=rsem,
            device_id={"seq": dev}, device_id_type=MESH,
        )

    part = rows // 2
    quarter = rows // 4
    tail = seqs - 1
    pieces = [(part, quarter), (part + quarter, quarter), (0, part)]
    if pair:
        units = [(s, lo, part) for s in range(tail) for lo in (0, part)] + [(tail, lo, size) for lo, size in pieces]
    else:
        units = [None]
    stride = len(units) + 1

    def strip(block, lo, size):
        return buf.at[block, pl.ds(lo, size), :]

    def own_unit(dev, i):
        if not pair:
            return buf.at[pl.ds(dev * seqs, seqs)]
        return strip(dev * seqs + units[i][0], units[i][1], units[i][2])

    def extra_unit(zz):
        return strip((zz * across + across - 1 - y) * seqs + tail, 0, part)

    def up(ref, k, i, dev):
        return send(ref, ref, us_sem.at[k * stride + i], ur_sem.at[k * stride + i], dev)

    def down(ref, k, i, dev):
        return send(ref, ref, ds_sem.at[k * stride + i], dr_sem.at[k * stride + i], dev)

    def id_up(zz, k, dev):
        ref = table_all.at[y, zz]
        return send(ref, ref, is_sem.at[k], ir_sem.at[k], dev)

    def id_down(zz, k, dev):
        ref = table_all.at[y, zz]
        return send(ref, ref, is_sem.at[depth + k], ir_sem.at[depth + k], dev)

    def id_side(yy):
        ref = table_all.at[yy]
        return send(ref, ref, is_sem.at[2 * depth], ir_sem.at[2 * depth], y_peer)

    def tail_side(dev):
        ref = strip(dev * seqs + tail, 0, part)
        return send(ref, ref, ys_sem.at[3 * slots], yr_sem.at[3 * slots], y_peer)

    def cross_pieces(h, j):
        if h == 0:
            return [(0, part)]
        if j < slots - 1:
            return [(part, part)]
        return [(part, quarter), (part + quarter, quarter)]

    def cross_send(j, lo, size):
        i = 3 * j + (0 if lo == 0 else 1 if lo == part else 2)
        cut = pl.ds(lo, size)
        return send(
            cross.at[j, cut, :], buf.at[n * seqs + j, cut, :], ys_sem.at[i], yr_sem.at[i], y_peer,
        )

    all_cross = [(j, lo, size) for j in range(slots) for h in range(2) for lo, size in cross_pieces(h, j)]

    def id_scalar(yy, zz, i):
        return pltpu.make_async_copy(table_all.at[yy, zz], table_s.at[yy, zz], t_sem.at[i])

    def send_own(i):
        @pl.when(has_down)
        def _():
            down(own_unit(me, i), 0, i, me - across).start()

        @pl.when(has_up)
        def _():
            up(own_unit(me, i), 0, i, me + across).start()

    def send_ids():
        @pl.when(has_down)
        def _():
            id_down(z, 0, me - across).start()

        @pl.when(has_up)
        def _():
            pl.semaphore_wait(in_up, 1)
            id_up(z, 0, me + across).start()

    def project(s):
        acc = jnp.zeros((rows, w_buf.shape[2]), jnp.float32)
        squares = jnp.zeros((rows, HD), jnp.float32)
        own_copies[s].wait()
        for slot in range(PIECES):
            if slot >= per_half:
                peer_copies[s][slot - per_half].wait_recv()
            if s == 0:
                w_copies[slot].wait()
            src = h_own if slot < per_half else h_peer
            half_of = side if slot < per_half else 1 - side
            at = (slot % per_half) * piece
            raw = src[s, :, pl.ds(at, piece)]
            wide = raw.astype(jnp.float32)
            sq = wide * wide
            for j in range(piece // HD):
                squares = squares + sq[:, j * HD:(j + 1) * HD]
            scaled = (wide * gain[pl.ds(half_of * local + at, piece)].astype(jnp.float32).reshape(1, piece)).astype(jnp.bfloat16)
            acc = acc + jnp.dot(scaled, w_buf[slot], preferred_element_type=jnp.float32)
        total = jnp.sum(squares, axis=1, keepdims=True)
        acc = acc * lax.rsqrt(total / full + epsilon)
        living = position < lengths[s]
        for col in range(0, acc.shape[1], 2 * HD):
            key = acc[:, col:col + HD]
            value = acc[:, col + HD:col + 2 * HD]
            turned = key * cosine + pltpu.roll(key, HD // 2, 1) * sine
            buf[me * seqs + s, :, col:col + HD] = jnp.where(living, turned, 0.0).astype(jnp.bfloat16)
            buf[me * seqs + s, :, col + HD:col + 2 * HD] = jnp.where(living, value, 0.0).astype(jnp.bfloat16)

    def settle(ks):
        for k in ks:
            @pl.when(has_up & (z - k >= 0))
            def _():
                id_up(z - k, k, me + across).wait_send()
                for i in range(len(units)):
                    up(own_unit(me - k * across, i), k, i, me + across).wait_send()

            @pl.when(has_down & (z + k < depth))
            def _():
                id_down(z + k, k, me - across).wait_send()
                for i in range(len(units)):
                    down(own_unit(me + k * across, i), k, i, me - across).wait_send()

    smalls[2].wait()
    smalls[3].wait()
    at_edge = (z == 0) | (z == depth - 1)
    for s in range(seqs):
        project(s)
        if s == 0:
            send_ids()
        if pair:
            if s == tail:
                @pl.when(y == 0)
                def _():
                    pl.semaphore_wait(in_side, 1)

                @pl.when(at_edge & twice)
                def _():
                    tail_side(me).start()
            mine = [i for i, unit in enumerate(units) if unit[0] == s]
            if s < tail:
                for i in mine:
                    send_own(i)
            else:
                for when, order in ((at_edge, mine), (jnp.logical_not(at_edge), mine[-1:] + mine[:-1])):
                    @pl.when(when)
                    def _():
                        for i in order:
                            send_own(i)
    if not pair:
        send_own(0)
    for s in range(seqs):
        for c in peer_copies[s]:
            c.wait_send()
    own_scalar = id_scalar(y, z, 2 * depth)
    own_scalar.start()

    if pair:
        @pl.when(at_edge & twice)
        def _():
            tail_side(y_peer).wait_recv()

        @pl.when((z == 0) & twice)
        def _():
            up(extra_unit(0), 0, stride - 1, me + across).start()

        @pl.when((z == depth - 1) & twice)
        def _():
            down(extra_unit(depth - 1), 0, stride - 1, me - across).start()

    own_scalar.wait()

    if not pair:
        for k in range(depth - 1):
            @pl.when(z - 1 - k >= 0)
            def _():
                id_up(z - 1 - k, k, me - across).wait_recv()
                if k + 1 < depth - 1:
                    @pl.when(has_up)
                    def _():
                        id_up(z - 1 - k, k + 1, me + across).start()
                up(own_unit(me - (k + 1), 0), k, 0, me - across).wait_recv()
                if k + 1 < depth - 1:
                    @pl.when(has_up)
                    def _():
                        up(own_unit(me - (k + 1), 0), k + 1, 0, me + across).start()

            @pl.when(z + 1 + k < depth)
            def _():
                id_down(z + 1 + k, k, me + across).wait_recv()
                if k + 1 < depth - 1:
                    @pl.when(has_down)
                    def _():
                        id_down(z + 1 + k, k + 1, me - across).start()
                down(own_unit(me + (k + 1), 0), k, 0, me + across).wait_recv()
                if k + 1 < depth - 1:
                    @pl.when(has_down)
                    def _():
                        down(own_unit(me + (k + 1), 0), k + 1, 0, me - across).start()

        to_scalar = pltpu.make_async_copy(table_all, table_s, t_sem.at[0])
        to_scalar.start()
        to_scalar.wait()

        def look(dev, found):
            for s in range(seqs):
                page = table_s[0, dev, 0, s]
                found = tuple(
                    jnp.where(page == me * SLOTS + j, dev * seqs + s, f) for j, f in enumerate(found)
                )
            return found

        found = lax.fori_loop(0, n, look, (jnp.int32(-1),) * SLOTS)
        where_is = [found, found]
    else:
        total = seqs * depth
        near = jnp.minimum(z, depth - 1 - z)
        below_far = z > depth - 1 - z
        first_pop = [total - slots - twice.astype(jnp.int32), total - slots]

        def arrival(a):
            if a < seqs:
                return z, jnp.int32(a), z >= depth, jnp.int32(0)
            i = a - seqs
            both = i < near * 2 * seqs
            rest = i - near * 2 * seqs
            k = jnp.where(both, i // (2 * seqs), near + rest // seqs)
            s = jnp.where(both, (i % (2 * seqs)) // 2, rest % seqs)
            below = (both & (i % 2 == 0)) | (jnp.logical_not(both) & below_far)
            zz = jnp.where(below, z - 1 - k, z + 1 + k)
            return zz, s, below, k

        arrivals = [arrival(a) for a in range(total)]

        def is_tail(a):
            zz, s, _, _ = arrivals[a]
            return ((zz == 0) | (zz == depth - 1)) & (s == tail) & twice

        def queue(lane_of, a, target, last, places):
            zz, s, _, _ = arrivals[a]
            page = table_s[lane_of, zz, 0, s]
            wanted = (page >= target * SLOTS) & (page < target * SLOTS + SLOTS)
            for h in range(2):
                goes = wanted & jnp.logical_not(is_tail(a)) if h == 0 else wanted
                place = jnp.maximum(last[h] + 1, jnp.maximum(a - first_pop[h], 0))
                places[h].append(jnp.where(goes, place, -1))
                last[h] = jnp.where(goes, place, last[h])

        def pop(h, a, places, cuts=None):
            top = a - (total - slots)
            if top < 0 and (h == 1 or top < -1):
                return
            j = jnp.int32(a) - first_pop[h]

            def fill():
                for lo, size in cuts or cross_pieces(h, top):
                    cut = pl.ds(lo, size)
                    content = None
                    for c in range(max(top, 0), a + 1):
                        zz, s, _, _ = arrivals[c]
                        rows_c = buf[(zz * across + y) * seqs + s, cut, :]
                        content = rows_c if content is None else jnp.where(places[h][c] == j, rows_c, content)
                    cross[j, cut, :] = content
                    cross_send(j, lo, size).start()

            if h == 0 and top < 0:
                pl.when(twice)(fill)
            elif h == 0 and a == total - 1:
                pl.when(jnp.logical_not(twice))(fill)
            else:
                fill()

        def relay(a, when, i, lo, size):
            zz, s, below, k = arrivals[a]
            ref = strip((zz * across + y) * seqs + s, lo, size)

            @pl.when(when & below)
            def _():
                up(ref, k, i, me - across).wait_recv()

                @pl.when(has_up)
                def _():
                    up(ref, k + 1, i, me + across).start()

            @pl.when(when & jnp.logical_not(below))
            def _():
                down(ref, k, i, me + across).wait_recv()

                @pl.when(has_down)
                def _():
                    down(ref, k + 1, i, me - across).start()

        def relay_id(a):
            zz, s, below, k = arrivals[a]

            @pl.when(below & (s == 0))
            def _():
                id_up(zz, k, me - across).wait_recv()

                @pl.when(has_up)
                def _():
                    id_up(zz, k + 1, me + across).start()

            @pl.when(jnp.logical_not(below) & (s == 0))
            def _():
                id_down(zz, k, me + across).wait_recv()

                @pl.when(has_down)
                def _():
                    id_down(zz, k + 1, me - across).start()

            @pl.when(s == 0)
            def _():
                id_scalar(y, zz, zz).start()

        def relay_extra(a):
            zz, s, below, k = arrivals[a]

            @pl.when(is_tail(a) & below)
            def _():
                up(extra_unit(zz), k, stride - 1, me - across).wait_recv()

                @pl.when(has_up)
                def _():
                    up(extra_unit(zz), k + 1, stride - 1, me + across).start()

            @pl.when(is_tail(a) & jnp.logical_not(below))
            def _():
                down(extra_unit(zz), k, stride - 1, me + across).wait_recv()

                @pl.when(has_down)
                def _():
                    down(extra_unit(zz), k + 1, stride - 1, me - across).start()

        last = [jnp.int32(-1), jnp.int32(-1)]
        places = [[], []]
        for a in range(seqs):
            queue(y, a, y_peer, last, places)
        for a in range(seqs, total):
            zz, s, _, _ = arrivals[a]
            relay_id(a)
            ending = a == total - 1
            if not ending:
                relay(a, s < tail, 2 * s, 0, part)
                relay(a, s == tail, stride - 2, 0, part)

            @pl.when(s == 0)
            def _():
                id_scalar(y, zz, zz).wait()

            queue(y, a, y_peer, last, places)
            if a == total - seqs:
                id_side(y).start()
            if not ending:
                pop(0, a, places)
                relay(a, s < tail, 2 * s + 1, part, part)
            for t, (lo, size) in enumerate(pieces):
                if ending or lo:
                    relay(a, s == tail, 2 * tail + t, lo, size)
                if ending:
                    pop(1 if lo else 0, a, places, [(lo, size)])
            if not ending:
                pop(1, a, places)
            relay_extra(a)
            if a == total - 2:
                id_side(1 - y).wait_recv()
                rest = pltpu.make_async_copy(table_all.at[1 - y], table_s.at[1 - y], t_sem.at[2 * depth + 1])
                rest.start()
                rest.wait()
                found = [[jnp.int32(-1)] * SLOTS for _ in range(2)]
                peer_last = [jnp.int32(-1), jnp.int32(-1)]
                peer_places = [[], []]
                for c in range(total):
                    cz, cs, _, _ = arrivals[c]
                    queue(1 - y, c, me, peer_last, peer_places)
                    mine = table_s[y, cz, 0, cs] - me * SLOTS
                    theirs = table_s[1 - y, cz, 0, cs] - me * SLOTS
                    here = (cz * across + y) * seqs + cs
                    there = (cz * across + 1 - y) * seqs + cs
                    for h in range(2):
                        place = n * seqs + peer_places[h][c]
                        if h == 0:
                            place = jnp.where(is_tail(c), there, place)
                        found[h] = [
                            jnp.where(mine == j, here, jnp.where(theirs == j, place, f))
                            for j, f in enumerate(found[h])
                        ]
                where_is = found
                settle(range(depth - 2))
        for piece_of in all_cross:
            cross_send(*piece_of).wait_recv()

    for h in range(2):
        cut = pl.ds(h * part, part)
        for j in range(SLOTS):
            index = where_is[h][j]
            rows_j = buf[jnp.maximum(index, 0), cut, :]
            out[j, cut, :] = jnp.where(index >= 0, rows_j, jnp.zeros_like(rows_j))

    settle(range(depth - 2, depth - 1) if pair else range(depth - 1))
    if pair:
        @pl.when(has_up & twice)
        def _():
            up(extra_unit(0), z, stride - 1, me + across).wait_send()

        @pl.when(has_down & twice)
        def _():
            down(extra_unit(depth - 1), depth - 1 - z, stride - 1, me - across).wait_send()

        @pl.when(at_edge & twice)
        def _():
            tail_side(me).wait_send()

        id_side(y).wait_send()
        for piece_of in all_cross:
            cross_send(*piece_of).wait_send()


def solution(mesh):
    n = mesh.shape["seq"]

    def per_device(hidden, norm_gain, w_kv, lengths, page_table):
        seqs, rows, local = hidden.shape
        full, width = w_kv.shape
        assert rows == BLOCK and page_table.shape == (seqs, 1)
        wide = mesh.shape["group"] * 2 == PLANE and n % 2 == 0 and seqs * (n // 2) > SLOTS
        across = 2 if wide else 1
        depth = n // across
        slots = SLOTS if wide else 0
        piece = full // PIECES
        half_dim = HD // 2
        inv_freq = np.power(np.float64(rope_base), -2.0 * np.arange(half_dim) / HD)
        freq = jnp.asarray(np.tile(inv_freq, 2)[None, :].astype(np.float32))
        stride = (2 * seqs + 1 if wide else 1) + 1
        z_sems = pltpu.SemaphoreType.DMA((max(1, (depth - 1) * stride),))
        y_sems = pltpu.SemaphoreType.DMA((3 * slots + 1,))
        vmem = pl.BlockSpec(memory_space=pltpu.VMEM)
        hbm = pl.BlockSpec(memory_space=pltpu.HBM)
        return pl.pallas_call(
            functools.partial(kernel, depth, across, slots),
            out_shape=pltpu.VMEM((SLOTS, BLOCK, width), jnp.bfloat16),
            in_specs=[hbm] * 6,
            out_specs=vmem,
            scratch_shapes=[
                pltpu.VMEM((seqs, rows, local), jnp.bfloat16),
                pltpu.VMEM((seqs, rows, local), jnp.bfloat16),
                pltpu.VMEM((PIECES, piece, width), jnp.bfloat16),
                pltpu.VMEM((n * seqs + slots, rows, width), jnp.bfloat16),
                pltpu.VMEM((max(1, slots), rows, width), jnp.bfloat16),
                pltpu.VMEM((full,), jnp.bfloat16),
                pltpu.VMEM((1, HD), jnp.float32),
                pltpu.SMEM((seqs,), jnp.int32),
                pltpu.SMEM((seqs,), jnp.int32),
                pltpu.VMEM((across, depth, 1, HD), jnp.int32),
                pltpu.SMEM((across, depth, 1, HD), jnp.int32),
                pltpu.SemaphoreType.DMA((seqs,)),
                pltpu.SemaphoreType.DMA((seqs * PIECES // 2,)),
                pltpu.SemaphoreType.DMA((seqs * PIECES // 2,)),
                pltpu.SemaphoreType.DMA((PIECES,)),
                pltpu.SemaphoreType.DMA((4,)),
                pltpu.SemaphoreType.DMA((2 * depth + 1,)),
                pltpu.SemaphoreType.DMA((2 * depth + 1,)),
                pltpu.SemaphoreType.DMA((2 * depth + 2,)),
                z_sems, z_sems, z_sems, z_sems, y_sems, y_sems,
                pltpu.SemaphoreType.REGULAR,
                pltpu.SemaphoreType.REGULAR,
            ],
            compiler_params=pltpu.CompilerParams(collective_id=0, has_side_effects=True, vmem_limit_bytes=63 * 1000 * 1024),
        )(hidden, norm_gain, w_kv, lengths, page_table.reshape(seqs), freq)

    return jax.shard_map(
        per_device,
        mesh=mesh,
        in_specs=(P("group", "seq", "tensor"), P(), P(None, "tensor"), P("group"), P("group", "seq")),
        out_specs=P(("group", "seq"), None, "tensor"),
        check_vma=False,
    )
```
